8 devices in a mesh: dp: 1 (over z), tp: 8 (over x, y, core).
Axes of the slice: x: 2, y: 2, z: 1, core: 2. Of those that a mesh axis runs over, the one named last changes fastest.
Arguments:
- x: bfloat16 [1024, 16384], P(('dp', 'tp'))
- gain: bfloat16 [16384], replicated
- wq: bfloat16 [16384, 16384], P(None, 'tp')
- wk: bfloat16 [16384, 16384], P(None, 'tp')
- wv: bfloat16 [16384, 16384], P(None, 'tp')
- wo: bfloat16 [16384, 16384], P('tp')
Outputs:
- output: bfloat16 [1024, 16384], P(('dp', 'tp'))
All inputs are finite; a program needn't handle non-finite values.
Results may differ from the reference program's by a relative error of at most 0.012.
Values are sent between devices in bfloat16 or wider.
A program may use at most 2 GiB of HBM per device.

```python
import jax
import jax.numpy as jnp
from jax import lax

ROWS = 1024
D = 16384
HEADS = 128
KV_HEADS = 128
HEAD = 128
THETA = 10000


def setup_inputs(seed: int = 0, part: int = 0) -> dict:
    kx, kn, kq, kk, kv, ko = jax.random.split(jax.random.key(seed), 6)

    def weights(key, rows, columns):
        return jax.random.normal(key, (rows, columns), jnp.float32) * rows**-0.5

    drawn = {
        "x": jax.random.normal(jax.random.fold_in(kx, part), (ROWS, D), jnp.float32),
        "gain": 1 + 0.1 * jax.random.normal(kn, (D,), jnp.float32),
        "wq": 2 * weights(kq, D, HEADS * HEAD),
        "wk": 2 * weights(kk, D, KV_HEADS * HEAD),
        "wv": 4 * weights(kv, D, KV_HEADS * HEAD),
        "wo": weights(ko, HEADS * HEAD, D),
    }
    return {k: v.astype(jnp.bfloat16) for k, v in drawn.items()}


def normed(x, gain):
    wide = x.astype(jnp.float32)
    scale = lax.rsqrt(jnp.mean(wide * wide, -1, keepdims=True) + 1e-6)
    return (wide * scale * gain.astype(jnp.float32)).astype(jnp.bfloat16)


def turned(t, place, theta):
    half = t.shape[-1] // 2
    angle = place.astype(jnp.float32)[:, None] * theta ** (-jnp.arange(half, dtype=jnp.float32) / half)
    cos, sin = jnp.cos(angle)[:, None], jnp.sin(angle)[:, None]
    a, b = t[..., :half].astype(jnp.float32), t[..., half:].astype(jnp.float32)
    return jnp.concatenate([a * cos - b * sin, b * cos + a * sin], -1).astype(jnp.bfloat16)


def matmul(a, w):
    return jnp.dot(a, w, preferred_element_type=jnp.float32).astype(jnp.bfloat16)


def einsum(form, a, b):
    return jnp.einsum(form, a.astype(jnp.float32), b.astype(jnp.float32))


def attention(q, k, v):
    scores = einsum("tgsd,ugd->gstu", q, k) * q.shape[-1] ** -0.5
    token = jnp.arange(q.shape[0])
    scores = jnp.where(token[:, None] >= token, scores, -jnp.inf)
    weights = jax.nn.softmax(scores, -1).astype(jnp.bfloat16)
    return einsum("gstu,ugd->tgsd", weights, v).astype(jnp.bfloat16)


def reference(x, gain, wq, wk, wv, wo):
    a, place = normed(x, gain), jnp.arange(ROWS)
    q = turned(matmul(a, wq).reshape(ROWS, HEADS, HEAD), place, THETA).reshape(ROWS, KV_HEADS, -1, HEAD)
    k = turned(matmul(a, wk).reshape(ROWS, KV_HEADS, HEAD), place, THETA)
    v = matmul(a, wv).reshape(ROWS, KV_HEADS, HEAD)
    seen = attention(q, k, v).reshape(ROWS, HEADS * HEAD)
    return (x.astype(jnp.float32) + jnp.dot(seen, wo, preferred_element_type=jnp.float32)).astype(jnp.bfloat16)
```

```python
import jax
import jax.numpy as jnp
from jax import lax
from jax.experimental import pallas as pl
from jax.experimental.pallas import tpu as pltpu
from jax.sharding import PartitionSpec as P


BF, F32 = jnp.bfloat16, jnp.float32
HEAD = 128
THETA = 10000
ROWS = 128
TK, TN = 2048, 1024
SLOTS = 4
LAG = 3
RING = 8
NEG = -1e30
MESH = pl.DeviceIdType.MESH
VMEM = 67_000_000


def place(stage, core, x, y):
    fx = (stage // 2) * core + (stage % 2) * (1 - core)
    fy = (stage // 2) * (1 - core) + (stage % 2) * core
    return (x + fx - 2 * x * fx) * 2 + y + fy - 2 * y * fy, core


def here():
    t = lax.axis_index("tp")
    return t // 4, (t // 2) % 2, t % 2


def dev(x, y, core):
    return {"tp": (x * 2 + y) * 2 + core}


def partners():
    x, y, c = here()
    first = dev(x + (1 - c) * (1 - 2 * x), y + c * (1 - 2 * y), c)
    second = dev(x + c * (1 - 2 * x), y + (1 - c) * (1 - 2 * y), c)
    return dev(x, y, 1 - c), first, second


def meet(others):
    barrier = pltpu.get_barrier_semaphore()
    for o in others:
        pl.semaphore_signal(barrier, inc=1, device_id=o, device_id_type=MESH)
    pl.semaphore_wait(barrier, len(others))


def send(src, dst, sems, i, to):
    return pltpu.make_async_remote_copy(src_ref=src, dst_ref=dst, send_sem=sems[0].at[i], recv_sem=sems[1].at[i], device_id=to, device_id_type=MESH)


def turn(t, cs, sn):
    return (t * cs + pltpu.roll(t, HEAD // 2, 1) * sn).astype(BF)


def rounded(t):
    return t.astype(BF).astype(F32)


def gather_project(x_ref, cs_ref, sn_ref, wq, wk, wv, k_out, v_out, q_out, x_out, xv, wb, acc, stage, w_sem, o_sem, x_sem, l_sem, s_sem, r_sem):
    x, y, c = here()
    other, first, second = partners()
    depth = wk.shape[0]
    per = depth // TK
    heads = TN // HEAD
    halves = wk.shape[1] // TN
    groups = [3 * halves] + [2 * halves] * 3
    total = sum(groups) * per

    def what(g):
        late = jnp.maximum(g - groups[0], 0)
        m = jnp.where(g < groups[0], g // halves, (late // halves) % 2)
        return m, g % halves

    def weights(b, start):
        g, k = b // per, b % per
        m, n = what(g)
        at = lambda w: w.at[pl.ds(pl.multiple_of(k * TK, TK), TK), pl.ds(pl.multiple_of(n * TN, TN), TN)]
        slot = b % SLOTS
        if not start:
            pltpu.make_async_copy(at(wk), wb.at[slot], w_sem.at[slot]).wait()
            return
        for i, w in enumerate((wk, wv, wq)):
            @pl.when(m == i)
            def _():
                pltpu.make_async_copy(at(w), wb.at[slot], w_sem.at[slot]).start()

    meet((other, first, second))
    sems = (s_sem, r_sem)
    mine = lambda s: xv.at[s, pl.ds(0, ROWS)]
    theirs = lambda s: xv.at[s, pl.ds(ROWS, ROWS)]
    share = [send(x_ref if s == 0 else mine(s), theirs(s), sems, s, other) for s in range(4)]
    hop = [None, send(x_ref, mine(1), sems, 4, first), send(x_ref, mine(2), sems, 5, second), send(mine(1), mine(3), sems, 6, second)]
    load = pltpu.make_async_copy(x_ref, mine(0), l_sem)
    hop[1].start()
    share[0].start()
    load.start()
    for b in range(SLOTS):
        weights(b, True)
    acc[...] = jnp.zeros_like(acc)

    def keep(s, p):
        return pltpu.make_async_copy(xv.at[s, pl.ds(p * ROWS, ROWS)], x_out.at[s - 1, pl.ds(p * ROWS, ROWS)], x_sem.at[2 * s - 2 + p])

    def out(g, s, p, ref):
        m, n = what(g)
        chip, core = place(s, c if p == 0 else 1 - c, x, y)
        token = pl.multiple_of((2 * chip + core) * ROWS, ROWS)
        row = p * ROWS if ref is q_out else token
        return pltpu.make_async_copy(stage.at[g % 2, :, pl.ds(p * ROWS, ROWS)], ref.at[pl.ds(n * heads, heads), pl.ds(row, ROWS)], o_sem.at[g % 2, p])

    def run(s, lo, hi):
        def step(b, _):
            g, k = b // per, b % per
            weights(b, False)
            acc[...] += jnp.dot(xv[s, :, pl.ds(pl.multiple_of(k * TK, TK), TK)], wb[b % SLOTS], preferred_element_type=F32)

            @pl.when(b + SLOTS < total)
            def _():
                weights(b + SLOTS, True)

            @pl.when(k == per - 1)
            def _():
                m, n = what(g)

                @pl.when(g >= 2)
                def _():
                    for p in range(2):
                        out(g, s, p, k_out).wait()

                @pl.when(m == 1)
                def _():
                    for h in range(heads):
                        stage[g % 2, h] = acc[:, h * HEAD : (h + 1) * HEAD].astype(BF)

                @pl.when(m != 1)
                def _():
                    for h in range(heads):
                        stage[g % 2, h] = turn(rounded(acc[:, h * HEAD : (h + 1) * HEAD]), cs_ref[s], sn_ref[s])

                acc[...] = jnp.zeros_like(acc)
                for i, ref in enumerate((k_out, v_out, q_out)):
                    if i == 2 and s:
                        continue

                    @pl.when(m == i)
                    def _():
                        for p in range(2):
                            out(g, s, p, ref).start()

            return 0

        lax.fori_loop(lo, hi, step, 0)

    ends = [sum(groups[: s + 1]) * per for s in range(4)]
    load.wait()
    share[0].wait_recv()
    run(0, 0, FIRST)
    hop[1].wait_send()
    hop[2].start()
    hop[1].wait_recv()
    share[1].start()
    keep(1, 0).start()
    run(0, FIRST, ends[0])
    share[1].wait_recv()
    keep(1, 1).start()
    run(1, ends[0], SECOND)
    hop[2].wait_send()
    hop[3].start()
    hop[2].wait_recv()
    share[2].start()
    keep(2, 0).start()
    run(1, SECOND, ends[1])
    share[2].wait_recv()
    keep(2, 1).start()
    run(2, ends[1], ends[2])
    hop[3].wait_recv()
    share[3].start()
    keep(3, 0).start()
    share[3].wait_recv()
    keep(3, 1).start()
    run(3, ends[2], ends[3])
    hop[3].wait_send()
    for s in range(4):
        share[s].wait_send()
    for s in range(1, 4):
        for p in range(2):
            keep(s, p).wait()
    for g in (sum(groups) - 2, sum(groups) - 1):
        for p in range(2):
            out(g, 3, p, k_out).wait()


FIRST, SECOND = 34, 72


def attend_scatter(x_ref, xs, q_in, k_in, v_in, cs_ref, sn_ref, wq, wo, y_out, xc, ks, vs, qs, seen, acc, wb, mine, away, near, total, got, w_sem,
                   x_sem, l_sem, y_sem, a_sem, n_sem, t_sem, g_sem):
    x, y, c = here()
    other, first, second = partners()
    per = wq.shape[0] // TK
    heads = TN // HEAD
    halves = wq.shape[1] // TN
    tiles = wo.shape[1] // TN
    nq, nh = per * halves, ks.shape[0]
    count = 3 * (nq + tiles) + tiles
    low = HEAD**-0.5 * 1.4426950408889634

    def weights(b, start):
        slot = b % SLOTS
        copy = lambda src: pltpu.make_async_copy(src, wb.at[slot], w_sem.at[slot])
        if not start:
            copy(wo.at[:, pl.ds(0, TN)]).wait()
            return
        late = b // (3 * (nq + tiles))
        r = b % (nq + tiles) + late * nq

        @pl.when(r < nq)
        def _():
            copy(wq.at[pl.ds(pl.multiple_of((r % per) * TK, TK), TK), pl.ds(pl.multiple_of((r // per % halves) * TN, TN), TN)]).start()

        @pl.when(r >= nq)
        def _():
            copy(wo.at[:, pl.ds(pl.multiple_of((r - nq) * TN, TN), TN)]).start()

    def chunk(s):
        return pltpu.make_async_copy(xs.at[2 - s], xc, x_sem)

    residual = pltpu.make_async_copy(x_ref, xc.at[pl.ds(0, ROWS)], x_sem)
    loads = [pltpu.make_async_copy(src, dst, l_sem.at[i]) for i, (src, dst) in enumerate(((k_in, ks), (v_in, vs), (q_in, qs.at[1])))]

    meet((other, first, second))
    chunk(0).start()
    for b in range(SLOTS):
        weights(b, True)
    for load in loads:
        load.start()
    acc[...] = jnp.zeros_like(acc)

    def project(s):
        chunk(s).wait()

        def half(n, _):
            def step(k, _):
                b = s * (nq + tiles) + n * per + k
                weights(b, False)
                acc[...] += jnp.dot(xc[:, pl.ds(pl.multiple_of(k * TK, TK), TK)], wb[b % SLOTS], preferred_element_type=F32)
                weights(b + SLOTS, True)
                return 0

            lax.fori_loop(0, per, step, 0)
            for h in range(heads):
                qs[0, n * heads + h] = turn(rounded(acc[:, h * HEAD : (h + 1) * HEAD]), cs_ref[3 - s], sn_ref[3 - s])
            acc[...] = jnp.zeros_like(acc)
            return 0

        lax.fori_loop(0, halves, half, 0)

    def attention(s):
        q_at = s // 3

        def block(p, _):
            chip, core = place(3 - s, c + p - 2 * c * p, x, y)
            rows = pl.ds(pl.multiple_of(p * ROWS, ROWS), ROWS)
            for n in range(4):
                @pl.when(chip == n)
                def _():
                    keys = (n + 1) * 2 * ROWS
                    late = (n * 2) * ROWS
                    ok = lax.broadcasted_iota(jnp.int32, (ROWS, 2 * ROWS), 1) <= lax.broadcasted_iota(jnp.int32, (ROWS, 2 * ROWS), 0) + core * ROWS

                    def some(i, _):
                        hs = [i * 4 + d for d in range(4)]
                        scores = []
                        for h in hs:
                            sc = lax.dot_general(qs[q_at, h, rows, :], ks[h, :keys, :], (((1,), (1,)), ((), ())), preferred_element_type=F32)
                            edge = jnp.where(ok, sc[:, late:], NEG)
                            scores.append(edge if n == 0 else jnp.concatenate([sc[:, :late], edge], 1))
                        for h, sc in zip(hs, scores):
                            w = jnp.exp2((sc - sc.max(1, keepdims=True)) * low)
                            sums = w.sum(1, keepdims=True)
                            o = jnp.dot(w.astype(BF), vs[h, :keys, :], preferred_element_type=F32)
                            seen[rows, pl.ds(pl.multiple_of(h * HEAD, HEAD), HEAD)] = (o * (1 / sums)).astype(BF)
                        return 0

                    lax.fori_loop(0, nh // 4, some, 0)

            return 0

        lax.fori_loop(0, 2, block, 0)

    def pair(s, j):
        return pltpu.make_async_remote_copy(src_ref=away.at[j % 4], dst_ref=near.at[j % RING], send_sem=a_sem.at[j % 4], recv_sem=n_sem.at[j % RING],
                                            device_id=other, device_id_type=MESH)

    def onward(s, q, to):
        return pltpu.make_async_remote_copy(src_ref=total.at[q], dst_ref=got.at[s, q], send_sem=t_sem.at[q], recv_sem=g_sem.at[s, q], device_id=to,
                                            device_id_type=MESH)

    def written(q):
        at = pl.ds(pl.multiple_of(q * TN, TN), TN)
        return pltpu.make_async_copy(xc.at[pl.ds(0, ROWS), at], y_out.at[:, at], y_sem.at[q])

    def scatter(s):
        def tile(j, _):
            @pl.when(j < tiles)
            def _():
                b = s * (nq + tiles) + nq * (1 - s // 3) + j
                weights(b, False)
                o = jnp.dot(seen[...], wb[b % SLOTS], preferred_element_type=F32)

                @pl.when(s * tiles + j >= 4)
                def _():
                    pair(s, j).wait_send()

                mine[j % (LAG + 1)] = o[:ROWS]
                away[j % 4] = o[ROWS:].astype(BF)
                pair(s, j).start()

                @pl.when(b + SLOTS < count)
                def _():
                    weights(b + SLOTS, True)

            @pl.when(j >= LAG)
            def _():
                q = j - LAG
                pair(s, q).wait_recv()
                t = mine.at[q % (LAG + 1)]
                there = near.at[q % RING]

                @pl.when((s == 1) | (s == 2))
                def _():
                    onward(0, q, first).wait_send()

                @pl.when(s < 2)
                def _():
                    total[q] = (t[...] + there[...].astype(F32)).astype(BF)

                @pl.when(s == 2)
                def _():
                    onward(0, q, second).wait_recv()
                    total[q] = (t[...] + there[...].astype(F32) + got[0, q].astype(F32)).astype(BF)
                    onward(2, q, first).start()

                for i in range(2):
                    @pl.when(s == i)
                    def _():
                        onward(i, q, second).start()

                @pl.when(s == 3)
                def _():
                    onward(1, q, second).wait_recv()
                    onward(2, q, first).wait_recv()
                    at = pl.ds(pl.multiple_of(q * TN, TN), TN)
                    sums = t[...] + there[...].astype(F32) + got[1, q].astype(F32) + got[2, q].astype(F32)
                    xc[:ROWS, at] = (xc[:ROWS, at].astype(F32) + sums).astype(BF)
                    written(q).start()

            return 0

        lax.fori_loop(0, tiles + LAG, tile, 0)

    def step(s, _):
        @pl.when(s < 3)
        def _():
            project(s)

        @pl.when(s < 2)
        def _():
            chunk(s + 1).start()

        @pl.when(s == 2)
        def _():
            residual.start()

        @pl.when(s == 0)
        def _():
            for load in loads:
                load.wait()

        attention(s)

        @pl.when(s == 3)
        def _():
            residual.wait()

        scatter(s)
        return 0

    lax.fori_loop(0, 4, step, 0)
    for j in range(4):
        pair(3, tiles - 4 + j).wait_send()

    def last(q, _):
        onward(2, q, first).wait_send()
        written(q).wait()
        return 0

    lax.fori_loop(0, tiles, last, 0)


def normed(x, gain):
    wide = x.astype(F32)
    scale = lax.rsqrt(jnp.mean(wide * wide, -1, keepdims=True) + 1e-6)
    return (wide * scale * gain.astype(F32)).astype(BF)


def tables():
    x, y, c = here()
    starts = []
    for s in range(4):
        for core in (c, 1 - c):
            chip, _ = place(s, core, x, y)
            starts.append((2 * chip + core) * ROWS)
    token = (jnp.stack(starts)[:, None] + jnp.arange(ROWS)).reshape(4, 2 * ROWS)
    half = HEAD // 2
    angle = token.astype(F32)[..., None] * THETA ** (-jnp.arange(half, dtype=F32) / half)
    cos, sin = jnp.cos(angle), jnp.sin(angle)
    return jnp.concatenate([cos, cos], -1), jnp.concatenate([-sin, sin], -1)


def solution(mesh):
    hbm = pl.BlockSpec(memory_space=pl.ANY)
    vmem = pl.BlockSpec(memory_space=pltpu.VMEM)
    dma = pltpu.SemaphoreType.DMA

    def step(x, gain, wq, wk, wv, wo):
        depth, width = wq.shape
        nh = width // HEAD
        tokens = 8 * ROWS
        tiles = depth // TN
        cs, sn = tables()
        shape = jax.ShapeDtypeStruct
        k, v, q, xs = pl.pallas_call(
            gather_project,
            out_shape=[shape((nh, tokens, HEAD), BF), shape((nh, tokens, HEAD), BF), shape((nh, 2 * ROWS, HEAD), BF), shape((3, 2 * ROWS, depth), BF)],
            in_specs=[hbm, vmem, vmem, hbm, hbm, hbm],
            out_specs=[hbm] * 4,
            scratch_shapes=[
                pltpu.VMEM((4, 2 * ROWS, depth), BF), pltpu.VMEM((SLOTS, TK, TN), BF), pltpu.VMEM((2 * ROWS, TN), F32),
                pltpu.VMEM((2, TN // HEAD, 2 * ROWS, HEAD), BF), dma((SLOTS,)), dma((2, 2)), dma((6,)), dma, dma((7,)), dma((7,)),
            ],
            compiler_params=pltpu.CompilerParams(collective_id=0, has_side_effects=True, vmem_limit_bytes=VMEM),
        )(normed(x, gain), cs, sn, wq, wk, wv)
        return pl.pallas_call(
            attend_scatter,
            out_shape=shape((ROWS, depth), BF),
            in_specs=[hbm] * 5 + [vmem, vmem, hbm, hbm],
            out_specs=hbm,
            scratch_shapes=[
                pltpu.VMEM((2 * ROWS, depth), BF), pltpu.VMEM((nh, tokens, HEAD), BF), pltpu.VMEM((nh, tokens, HEAD), BF),
                pltpu.VMEM((2, nh, 2 * ROWS, HEAD), BF), pltpu.VMEM((2 * ROWS, width), BF), pltpu.VMEM((2 * ROWS, TN), F32),
                pltpu.VMEM((SLOTS, TK, TN), BF), pltpu.VMEM((LAG + 1, ROWS, TN), F32), pltpu.VMEM((4, ROWS, TN), BF), pltpu.VMEM((RING, ROWS, TN), BF),
                pltpu.VMEM((tiles, ROWS, TN), BF), pltpu.VMEM((3, tiles, ROWS, TN), BF),
                dma((SLOTS,)), dma, dma((3,)), dma((tiles,)), dma((4,)), dma((RING,)), dma((tiles,)), dma((3, tiles)),
            ],
            compiler_params=pltpu.CompilerParams(collective_id=1, has_side_effects=True, vmem_limit_bytes=VMEM),
        )(x, xs, q, k, v, cs, sn, wq, wo)

    tokens, columns = P(("dp", "tp"), None), P(None, "tp")
    return jax.shard_map(
        step,
        mesh=mesh,
        in_specs=(tokens, P(None), columns, columns, columns, P("tp", None)),
        out_specs=tokens,
        check_vma=False,
    )
```

```python
import functools

import jax
import jax.numpy as jnp
import numpy as np
from jax import lax
from jax.experimental import pallas as pl
from jax.experimental.pallas import tpu as pltpu
from jax.sharding import PartitionSpec as P


BF, F32 = jnp.bfloat16, jnp.float32
HEAD = 128
THETA = 10000
ROWS = 128
TK, TN = 2048, 1024
SLOTS = 5
WIDE = 256
TALL = 3
LAG = 3
RING = 8
NEG = -1e30
MESH = pl.DeviceIdType.MESH
VMEM = 67_000_000


def place(stage, core, x, y):
    fx = (stage // 2) * core + (stage % 2) * (1 - core)
    fy = (stage // 2) * (1 - core) + (stage % 2) * core
    return (x + fx - 2 * x * fx) * 2 + y + fy - 2 * y * fy, core


def here():
    t = lax.axis_index("tp")
    return t // 4, (t // 2) % 2, t % 2


def dev(x, y, core):
    return {"tp": (x * 2 + y) * 2 + core}


def partners():
    x, y, c = here()
    first = dev(x + (1 - c) * (1 - 2 * x), y + c * (1 - 2 * y), c)
    second = dev(x + c * (1 - 2 * x), y + (1 - c) * (1 - 2 * y), c)
    return dev(x, y, 1 - c), first, second


def meet(others):
    barrier = pltpu.get_barrier_semaphore()
    for o in others:
        pl.semaphore_signal(barrier, inc=1, device_id=o, device_id_type=MESH)
    pl.semaphore_wait(barrier, len(others))


def send(src, dst, sems, i, to):
    return pltpu.make_async_remote_copy(src_ref=src, dst_ref=dst, send_sem=sems[0].at[i], recv_sem=sems[1].at[i], device_id=to, device_id_type=MESH)


def turn(t, cs, sn):
    return (t * cs + pltpu.roll(t, HEAD // 2, 1) * sn).astype(BF)


def rounded(t):
    return t.astype(BF).astype(F32)


def spread(tab_ref, cs, sn, stages):
    x, y, c = here()
    left = lax.broadcasted_iota(jnp.int32, (ROWS, HEAD), 1) < HEAD // 2
    for i, s in enumerate(stages):
        for p in range(2):
            chip, core = place(s, c + p - 2 * c * p, x, y)
            t = tab_ref[2 * chip + core]
            r = pltpu.roll(t, HEAD // 2, 1)
            cs[i, p * ROWS : (p + 1) * ROWS] = jnp.where(left, t, r)
            sn[i, p * ROWS : (p + 1) * ROWS] = jnp.where(left, -r, t)


def norm(ref, gain_ref, done):
    depth = ref.shape[1]
    wide = 1024

    def squares(i, total):
        t = ref[:, pl.ds(pl.multiple_of(i * wide, wide), wide)].astype(F32)
        t = t * t
        for n in range(0, wide, HEAD):
            total += t[:, n : n + HEAD]
        return total

    total = lax.fori_loop(0, depth // wide, squares, jnp.zeros((ROWS, HEAD), F32))
    scale = lax.rsqrt(total.sum(1, keepdims=True) / depth + 1e-6)

    def apply(i, _):
        at = pl.ds(pl.multiple_of(i * wide, wide), wide)
        ref[:, at] = (ref[:, at].astype(F32) * scale * gain_ref[:, at].astype(F32)).astype(BF)
        return 0

    for i in range(4):
        lax.fori_loop(i * depth // wide // 4, (i + 1) * depth // wide // 4, apply, 0)
        done(i)


def gather_project(x_ref, gain_ref, tab_ref, wq, wk, wv, k_out, v_out, q_out, x_out, xv, wb, made, stage, cs, sn, w_sem, o_sem, x_sem, l_sem, s_sem, r_sem):
    x, y, c = here()
    other, first, second = partners()
    depth = wk.shape[0]
    heads = WIDE // HEAD
    per = wk.shape[1] // WIDE
    total = 10 * per

    def what(g):
        m = g // per
        return m // 5 * 2 + m % 5 // 3, m % 5 % 3, g % per

    def weights(g, start):
        _, m, n = what(g)
        copy = lambda w: pltpu.make_async_copy(w.at[:, pl.ds(pl.multiple_of(n * WIDE, WIDE), WIDE)], wb.at[g % TALL], w_sem.at[g % TALL])
        if not start:
            copy(wk).wait()
            return
        for i, w in enumerate((wk, wv, wq)):
            @pl.when(m == i)
            def _():
                copy(w).start()

    mine = lambda s: xv.at[s, pl.ds(0, ROWS)]
    theirs = lambda s: xv.at[s, pl.ds(ROWS, ROWS)]
    load = pltpu.make_async_copy(x_ref, mine(0), l_sem)
    load.start()
    for g in range(TALL):
        weights(g, True)
    meet((other, first, second))
    sems = (s_sem, r_sem)
    part = lambda ref, i, of=2: ref.at[:, pl.ds(i * (depth // of), depth // of)]
    share = [None] + [send(mine(s), theirs(s), sems, s, other) for s in (1, 2)]
    share += [send(part(mine(3), i), part(theirs(3), i), sems, 3 + i, other) for i in range(2)]
    own = [send(part(mine(0), i, 4), part(theirs(0), i, 4), sems, 9 + i, other) for i in range(4)]
    hop = [None, send(mine(0), mine(1), sems, 5, first), send(mine(0), mine(2), sems, 6, second)]
    hop += [send(part(mine(1), i), part(mine(3), i), sems, 7 + i, second) for i in range(2)]
    load.wait()
    norm(mine(0), gain_ref, lambda i: own[i].start())
    hop[1].start()
    spread(tab_ref, cs, sn, range(4))

    def keep(s, p):
        return pltpu.make_async_copy(xv.at[s, pl.ds(p * ROWS, ROWS)], x_out.at[s // 2, pl.ds(p * ROWS, ROWS)], x_sem.at[s - 1 + p])

    def out(g, p, ref):
        s, _, n = what(g)
        chip, core = place(s, c if p == 0 else 1 - c, x, y)
        token = pl.multiple_of((2 * chip + core) * ROWS, ROWS)
        some = pl.ds(n * heads, heads)
        to = ref.at[s // 2, some, pl.ds(p * ROWS, ROWS)] if ref is q_out else ref.at[some, pl.ds(token, ROWS)]
        return pltpu.make_async_copy(stage.at[g % 2, :, pl.ds(p * ROWS, ROWS)], to, o_sem.at[g % 2, p])

    def stage_1():
        hop[1].wait_send()
        hop[2].start()
        hop[1].wait_recv()
        share[1].start()
        keep(1, 0).start()

    def stage_2():
        hop[2].wait_send()
        hop[3].start()
        hop[4].start()
        hop[2].wait_recv()
        share[2].start()

    def ready_1():
        share[1].wait_recv()
        keep(1, 1).start()

    def ready_2():
        share[2].wait_recv()

    def stage_3():
        hop[3].wait_recv()
        share[3].start()

    def stage_3_too():
        hop[4].wait_recv()
        share[4].start()
        keep(3, 0).start()

    def ready_3():
        share[3].wait_recv()
        share[4].wait_recv()
        keep(3, 1).start()

    events = {FIRST: stage_1, 3 * per: ready_1, SECOND: stage_2, 5 * per: ready_2, 6 * per: stage_3, 7 * per + per // 2: stage_3_too, 8 * per: ready_3}
    for copy in own:
        copy.wait_recv()

    def finish(g):
        s, m, _ = what(g)
        t = made[g % 2].astype(BF)
        for h in range(heads):
            th = t[:, h * HEAD : (h + 1) * HEAD]
            stage[g % 2, h] = jnp.where(m == 1, th, turn(th.astype(F32), cs[s], sn[s]))

    def leave(g):
        for i, ref in enumerate((k_out, v_out, q_out)):
            @pl.when(what(g)[1] == i)
            def _():
                for p in range(2):
                    out(g, p, ref).start()

    def step(g, _):
        for at, event in events.items():
            pl.when(g == at)(event)
        weights(g, False)
        before = jnp.maximum(g - 1, 0)

        @pl.when(g >= 3)
        def _():
            for p in range(2):
                out(before - 2, p, k_out).wait()

        finish(before)
        made[g % 2] = jnp.dot(xv[what(g)[0]], wb[g % TALL], preferred_element_type=F32)

        @pl.when(g + TALL < total)
        def _():
            weights(g + TALL, True)

        pl.when(g >= 1)(lambda: leave(before))
        return 0

    lax.fori_loop(0, total, step, 0)
    for p in range(2):
        out(total - 3, p, k_out).wait()
    finish(total - 1)
    leave(total - 1)
    for copy in (*own, *share[1:], *hop[3:]):
        copy.wait_send()
    for s in (1, 3):
        for p in range(2):
            keep(s, p).wait()
    for g in (total - 2, total - 1):
        for p in range(2):
            out(g, p, k_out).wait()


FIRST, SECOND = 17, 36


def attend_scatter(x_ref, xs, q_in, k_in, v_in, tab_ref, wq, wo, y_out, xc, ks, vs, qs, seen, wb, mine, away, near, total, got, made, cs, sn, w_sem, x_sem,
                   l_sem, y_sem, a_sem, n_sem, t_sem, g_sem):
    x, y, c = here()
    other, first, second = partners()
    heads = WIDE // HEAD
    cut = TN // WIDE
    per = wq.shape[0] // (TK * cut)
    nq = per * (wq.shape[1] // WIDE)
    tiles = wo.shape[1] // TN
    nh = ks.shape[0]
    count = 2 * nq + 4 * tiles
    low = HEAD**-0.5 * 1.4426950408889634

    def weights(b, start):
        slot = b % SLOTS
        tall = lambda j: pltpu.make_async_copy(wo.at[:, pl.ds(pl.multiple_of(j * TN, TN), TN)], wb.at[slot], w_sem.at[slot])
        if not start:
            tall(0).wait()
            return
        late = b // (2 * nq + 3 * tiles)
        r = (b + nq) % (nq + tiles) + late * nq

        @pl.when(r < nq)
        def _():
            columns = pl.ds(pl.multiple_of(r // per * WIDE, WIDE), WIDE)
            for i in range(cut):
                rows = pl.ds(pl.multiple_of((r % per * cut + i) * TK, TK), TK)
                pltpu.make_async_copy(wq.at[rows, columns], wb.at[slot, :, pl.ds(i * WIDE, WIDE)], w_sem.at[slot]).start()

        @pl.when(r >= nq)
        def _():
            tall(r - nq).start()

    def stage_of(i):
        return (1 - i // 2) * (2 + i) + i // 2 * (3 - i)

    def chunk(i):
        return pltpu.make_async_copy(xs.at[2 - i], xc, x_sem)

    residual = pltpu.make_async_copy(x_ref, xc.at[pl.ds(0, ROWS)], x_sem)
    loads = [pltpu.make_async_copy(src, dst, l_sem.at[i]) for i, (src, dst) in enumerate(((k_in, ks), (v_in, vs), (q_in, qs)))]

    for load in loads:
        load.start()
    for b in range(SLOTS):
        weights(b, True)
    chunk(1).start()
    meet((other, first, second))
    spread(tab_ref, cs, sn, (1, 3))

    def finish(s, n):
        for h in range(heads):
            qs[1, n * heads + h] = turn(rounded(made[n % 2, :, h * HEAD : (h + 1) * HEAD]), cs[2 - s], sn[2 - s])

    def project(s):
        chunk(s).wait()

        def tile(n, _):
            first_block = tiles + (s - 1) * (nq + tiles) + n * per
            blocks = [first_block + u for u in range(per)]
            for b in blocks:
                weights(b, False)
            finish(s, jnp.maximum(n - 1, 0))
            t = jnp.zeros((2 * ROWS, WIDE), F32)
            for u, b in enumerate(blocks):
                for i in range(cut):
                    at = (u * cut + i) * TK
                    t += jnp.dot(xc[:, at : at + TK], wb[b % SLOTS, :, i * WIDE : (i + 1) * WIDE], preferred_element_type=F32)
            made[n % 2] = t
            for b in blocks:
                weights(b + SLOTS, True)
            return 0

        lax.fori_loop(0, nq // per, tile, 0)
        finish(s, nq // per - 1)

    def attention(s):
        q_at = 1 - s // 3

        def block(p, _):
            chip, core = place(stage_of(s), c + p - 2 * c * p, x, y)
            rows = pl.ds(pl.multiple_of(p * ROWS, ROWS), ROWS)
            for n in range(4):
                @pl.when(chip == n)
                def _():
                    keys = (n + 1) * 2 * ROWS
                    late = (n * 2) * ROWS
                    ok = lax.broadcasted_iota(jnp.int32, (ROWS, 2 * ROWS), 1) <= lax.broadcasted_iota(jnp.int32, (ROWS, 2 * ROWS), 0) + core * ROWS

                    def some(i, _):
                        hs = [i * 4 + d for d in range(4)]
                        scores = []
                        for h in hs:
                            sc = lax.dot_general(qs[q_at, h, rows, :], ks[h, :keys, :], (((1,), (1,)), ((), ())), preferred_element_type=F32)
                            edge = jnp.where(ok, sc[:, late:], NEG)
                            scores.append(edge if n == 0 else jnp.concatenate([sc[:, :late], edge], 1))
                        for h, sc in zip(hs, scores):
                            w = jnp.exp2((sc - sc.max(1, keepdims=True)) * low)
                            sums = w.sum(1, keepdims=True)
                            o = jnp.dot(w.astype(BF), vs[h, :keys, :], preferred_element_type=F32)
                            seen[rows, pl.ds(pl.multiple_of(h * HEAD, HEAD), HEAD)] = (o * (1 / sums)).astype(BF)
                        return 0

                    lax.fori_loop(0, nh // 4, some, 0)

            return 0

        lax.fori_loop(0, 2, block, 0)

    def pair(j):
        return pltpu.make_async_remote_copy(src_ref=away.at[j % 4], dst_ref=near.at[j % RING], send_sem=a_sem.at[j % 4], recv_sem=n_sem.at[j % RING],
                                            device_id=other, device_id_type=MESH)

    def onward(s, q, to):
        return pltpu.make_async_remote_copy(src_ref=total.at[q], dst_ref=got.at[s, q], send_sem=t_sem.at[q], recv_sem=g_sem.at[s, q], device_id=to,
                                            device_id_type=MESH)

    def written(q):
        at = pl.ds(pl.multiple_of(q * TN, TN), TN)
        return pltpu.make_async_copy(xc.at[pl.ds(0, ROWS), at], y_out.at[:, at], y_sem.at[q])

    def scatter(s):
        base = (0, tiles + nq, 2 * (tiles + nq), 3 * tiles + 2 * nq)[s]

        def matmul(j):
            b = base + j
            o = jnp.dot(seen[...], wb[b % SLOTS], preferred_element_type=F32)
            mine[j % (LAG + 1)] = o[:ROWS]
            away[j % 4] = o[ROWS:].astype(BF)

        def before(j):
            weights(base + j, False)
            if s:
                pair(j).wait_send()
            else:
                pl.when(j >= 4)(lambda: pair(j).wait_send())

        def after(j):
            pair(j).start()
            b = base + j + SLOTS
            if s < 3:
                weights(b, True)
            else:
                pl.when(b < count)(lambda: weights(b, True))

        def arrive(q):
            pair(q).wait_recv()
            if s in (1, 2):
                onward(0, q, first).wait_send()
            if s == 2:
                onward(0, q, second).wait_recv()
            if s == 3:
                onward(1, q, second).wait_recv()
                onward(2, q, first).wait_recv()

        def add(q):
            t = mine[q % (LAG + 1)] + near[q % RING].astype(F32)
            if s == 2:
                t += got[0, q].astype(F32)
            if s < 3:
                total[q] = t.astype(BF)
                return
            t += got[1, q].astype(F32) + got[2, q].astype(F32)
            at = pl.ds(pl.multiple_of(q * TN, TN), TN)
            xc[:ROWS, at] = (xc[:ROWS, at].astype(F32) + t).astype(BF)

        def leave(q):
            if s < 3:
                onward((1, 0, 2)[s], q, first if s == 2 else second).start()
            else:
                written(q).start()

        def early(j, _):
            before(j)
            matmul(j)
            after(j)
            return 0

        def both(j, _):
            q = j - LAG
            before(j)
            arrive(q)
            add(q)
            matmul(j)
            leave(q)
            after(j)
            return 0

        def late(q, _):
            arrive(q)
            add(q)
            leave(q)
            return 0

        lax.fori_loop(0, LAG, early, 0)
        lax.fori_loop(LAG, tiles, both, 0)
        lax.fori_loop(tiles - LAG, tiles, late, 0)

    def step(s, _):
        @pl.when((s == 1) | (s == 2))
        def _():
            project(s)

        @pl.when(s == 1)
        def _():
            chunk(2).start()

        @pl.when(s == 2)
        def _():
            residual.start()

        @pl.when(s == 0)
        def _():
            for load in loads:
                load.wait()

        attention(s)

        @pl.when(s == 3)
        def _():
            residual.wait()

        for i in range(4):
            pl.when(s == i)(functools.partial(scatter, i))
        return 0

    lax.fori_loop(0, 4, step, 0)
    for j in range(4):
        pair(tiles - 4 + j).wait_send()

    def last(q, _):
        onward(2, q, first).wait_send()
        written(q).wait()
        return 0

    lax.fori_loop(0, tiles, last, 0)


def table(tokens):
    half = HEAD // 2
    angle = np.arange(tokens, dtype=np.float32)[:, None] * np.float32(THETA) ** (-np.arange(half, dtype=np.float32) / np.float32(half))
    return np.concatenate([np.cos(angle), np.sin(angle)], -1).astype(np.float32).reshape(-1, ROWS, HEAD)


def solution(mesh):
    hbm = pl.BlockSpec(memory_space=pl.ANY)
    vmem = pl.BlockSpec(memory_space=pltpu.VMEM)
    dma = pltpu.SemaphoreType.DMA

    def step(x, gain, wq, wk, wv, wo):
        depth, width = wq.shape
        nh = width // HEAD
        tokens = 8 * ROWS
        tiles = depth // TN
        tab = jnp.asarray(table(tokens))
        shape = jax.ShapeDtypeStruct
        k, v, q, xs = pl.pallas_call(
            gather_project,
            out_shape=[shape((nh, tokens, HEAD), BF), shape((nh, tokens, HEAD), BF), shape((2, nh, 2 * ROWS, HEAD), BF), shape((2, 2 * ROWS, depth), BF)],
            in_specs=[hbm, vmem, vmem, hbm, hbm, hbm],
            out_specs=[hbm] * 4,
            scratch_shapes=[
                pltpu.VMEM((4, 2 * ROWS, depth), BF), pltpu.VMEM((TALL, depth, WIDE), BF), pltpu.VMEM((2, 2 * ROWS, WIDE), F32),
                pltpu.VMEM((2, WIDE // HEAD, 2 * ROWS, HEAD), BF),
                pltpu.VMEM((4, 2 * ROWS, HEAD), F32), pltpu.VMEM((4, 2 * ROWS, HEAD), F32), dma((TALL,)), dma((2, 2)), dma((4,)), dma, dma((13,)), dma((13,)),
            ],
            compiler_params=pltpu.CompilerParams(collective_id=0, has_side_effects=True, vmem_limit_bytes=VMEM),
        )(x, gain[None], tab, wq, wk, wv)
        return pl.pallas_call(
            attend_scatter,
            out_shape=shape((ROWS, depth), BF),
            in_specs=[hbm] * 5 + [vmem, hbm, hbm],
            out_specs=hbm,
            scratch_shapes=[
                pltpu.VMEM((2 * ROWS, depth), BF), pltpu.VMEM((nh, tokens, HEAD), BF), pltpu.VMEM((nh, tokens, HEAD), BF),
                pltpu.VMEM((2, nh, 2 * ROWS, HEAD), BF), pltpu.VMEM((2 * ROWS, width), BF),
                pltpu.VMEM((SLOTS, TK, TN), BF), pltpu.VMEM((LAG + 1, ROWS, TN), F32), pltpu.VMEM((4, ROWS, TN), BF), pltpu.VMEM((RING, ROWS, TN), BF),
                pltpu.VMEM((tiles, ROWS, TN), BF), pltpu.VMEM((3, tiles, ROWS, TN), BF),
                pltpu.VMEM((2, 2 * ROWS, WIDE), F32), pltpu.VMEM((2, 2 * ROWS, HEAD), F32), pltpu.VMEM((2, 2 * ROWS, HEAD), F32),
                dma((SLOTS,)), dma, dma((3,)), dma((tiles,)), dma((4,)), dma((RING,)), dma((tiles,)), dma((3, tiles)),
            ],
            compiler_params=pltpu.CompilerParams(collective_id=1, has_side_effects=True, vmem_limit_bytes=VMEM),
        )(x, xs, q, k, v, tab, wq, wo)

    tokens, columns = P(("dp", "tp"), None), P(None, "tp")
    return jax.shard_map(
        step,
        mesh=mesh,
        in_specs=(tokens, P(None), columns, columns, columns, P("tp", None)),
        out_specs=tokens,
        check_vma=False,
    )
```
